32 devices in a mesh: dp: 4 (over y, z), pp: 8 (over x, core).
Axes of the slice: x: 4, y: 2, z: 2, core: 2. Of those that a mesh axis runs over, the one named last changes fastest.
The devices are a block of a 4x4x8 slice.
Arguments:
- x_in: bfloat16 [384, 1, 128, 128], P(('dp', 'pp')), parts along dimension 0
- dy_out: bfloat16 [384, 1, 128, 128], P(('dp', 'pp')), parts along dimension 0
- w_qkv: bfloat16 [8, 2, 1, 128, 3, 16, 8], P('pp')
- w_attn: bfloat16 [8, 2, 1, 16, 8, 128], P('pp')
- w_fc: bfloat16 [8, 2, 1, 128, 512], P('pp')
- w_proj: bfloat16 [8, 2, 1, 512, 128], P('pp')
- b_qkv: bfloat16 [8, 2, 1, 3, 16, 8], P('pp')
- b_fc: bfloat16 [8, 2, 1, 512], P('pp')
- vec_d: bfloat16 [8, 2, 1, 6, 128], P('pp')
Outputs:
- output 1: bfloat16 [384, 1, 128, 128], P(('dp', 'pp')), parts along dimension 0
- output 2: bfloat16 [384, 1, 128, 128], P(('dp', 'pp')), parts along dimension 0
- output 3: float32 [32, 2, 1, 128, 3, 16, 8], P(('dp', 'pp')), parts along dimension 0
- output 4: float32 [32, 2, 1, 16, 8, 128], P(('dp', 'pp')), parts along dimension 0
- output 5: float32 [32, 2, 1, 128, 512], P(('dp', 'pp')), parts along dimension 0
- output 6: float32 [32, 2, 1, 512, 128], P(('dp', 'pp')), parts along dimension 0
- output 7: float32 [32, 2, 1, 3, 16, 8], P(('dp', 'pp')), parts along dimension 0
- output 8: float32 [32, 2, 1, 512], P(('dp', 'pp')), parts along dimension 0
- output 9: float32 [32, 2, 1, 6, 128], P(('dp', 'pp')), parts along dimension 0
There are 4 independent parts. The reference program is written for one: setup_inputs(seed, part) draws one part's arguments, and reference() takes and returns one part's arrays. A program takes and returns all parts, laid end to end along the dimension named above; an argument that names none is the same for every part.
All inputs are finite; a program needn't handle non-finite values.
Results may differ from the reference program's by a relative error of at most 0.02.
Values are sent between devices in bfloat16 or wider.
A program may use at most 768 MiB of HBM per device.

```python
import jax
import jax.numpy as jnp
from jax import lax

STAGES = 8
MICRO = 96
LPS = 1
BATCH = 1
SEQ = 128
DM = 128
HEADS = 16
FF = 512
HEAD = DM // HEADS
LAYERS = STAGES * LPS
EPSILON = 1e-5


def with_second_copy(stage_major):
    return jnp.stack([stage_major, stage_major[::-1]], axis=1).astype(jnp.bfloat16)


def setup_inputs(seed: int = 0, part: int = 0) -> dict:
    root_key = jax.random.key(seed)
    data_keys = jax.random.split(jax.random.fold_in(root_key, part), 2)
    w_keys = jax.random.split(jax.random.key(seed + 7919), 7)
    res_scale = (2.0 * LAYERS) ** -0.5
    act_shape = (MICRO, BATCH, SEQ, DM)
    x_in = jax.random.normal(data_keys[0], act_shape, jnp.float32).astype(jnp.bfloat16)
    dy_out = jax.random.normal(data_keys[1], act_shape, jnp.float32).astype(jnp.bfloat16)
    w_qkv = with_second_copy(jax.random.normal(w_keys[0], (STAGES, LPS, DM, 3, HEADS, HEAD), jnp.float32) * DM ** -0.5)
    w_attn = with_second_copy(jax.random.normal(w_keys[1], (STAGES, LPS, HEADS, HEAD, DM), jnp.float32) * (DM ** -0.5 * res_scale))
    w_fc = with_second_copy(jax.random.normal(w_keys[2], (STAGES, LPS, DM, FF), jnp.float32) * DM ** -0.5)
    w_proj = with_second_copy(jax.random.normal(w_keys[3], (STAGES, LPS, FF, DM), jnp.float32) * (FF ** -0.5 * res_scale))
    b_qkv = with_second_copy(0.3 * jax.random.normal(w_keys[4], (STAGES, LPS, 3, HEADS, HEAD), jnp.float32))
    b_fc = with_second_copy(0.3 * jax.random.normal(w_keys[5], (STAGES, LPS, FF), jnp.float32))
    row_scale = jnp.array([0.2, 0.2, 0.5 * res_scale, 0.2, 0.2, 0.5 * res_scale], jnp.float32)
    row_shift = jnp.array([1.0, 0.0, 0.0, 1.0, 0.0, 0.0], jnp.float32)
    vec_rows = jax.random.normal(w_keys[6], (STAGES, LPS, 6, DM), jnp.float32)
    vec_d = with_second_copy(vec_rows * row_scale[:, None] + row_shift[:, None])
    return {'x_in': x_in, 'dy_out': dy_out, 'w_qkv': w_qkv, 'w_attn': w_attn, 'w_fc': w_fc, 'w_proj': w_proj, 'b_qkv': b_qkv, 'b_fc': b_fc, 'vec_d': vec_d}


def layer_norm(rows_in, ln_gain, ln_shift):
    rows_f32 = rows_in.astype(jnp.float32)
    row_mean = jnp.mean(rows_f32, axis=-1, keepdims=True)
    centered = rows_f32 - row_mean
    row_var = jnp.mean(centered * centered, axis=-1, keepdims=True)
    scaled = centered * lax.rsqrt(row_var + EPSILON)
    return (scaled * ln_gain.astype(jnp.float32) + ln_shift.astype(jnp.float32)).astype(jnp.bfloat16)


def gpt_layer(hidden_in, layer_w):
    w_qkv, w_attn, w_fc, w_proj, b_qkv, b_fc, vec_d = layer_w
    n_batch, seq_len, d_model = hidden_in.shape
    n_heads, head_dim = w_qkv.shape[-2], w_qkv.shape[-1]
    tokens = n_batch * seq_len
    flat_rows = hidden_in.reshape(tokens, d_model)
    normed = layer_norm(flat_rows, vec_d[0], vec_d[1])
    qkv_proj = jnp.dot(normed, w_qkv.reshape(d_model, 3 * d_model), preferred_element_type=jnp.float32)
    qkv_proj = (qkv_proj + b_qkv.reshape(3 * d_model).astype(jnp.float32)).astype(jnp.bfloat16)
    qkv_proj = qkv_proj.reshape(n_batch, seq_len, 3, n_heads, head_dim)
    query_heads = qkv_proj[:, :, 0].astype(jnp.float32)
    key_heads = qkv_proj[:, :, 1].astype(jnp.float32)
    value_heads = qkv_proj[:, :, 2].astype(jnp.float32)
    scores = jnp.einsum('bqhe,bkhe->bhqk', query_heads, key_heads) * (head_dim ** -0.5)
    causal = jnp.arange(seq_len)[:, None] >= jnp.arange(seq_len)[None, :]
    scores = jnp.where(causal, scores, -1e30)
    attn_probs = jax.nn.softmax(scores, axis=-1).astype(jnp.bfloat16)
    mixed_heads = jnp.einsum('bhqk,bkhe->bqhe', attn_probs.astype(jnp.float32), value_heads).astype(jnp.bfloat16)
    attn_out = jnp.dot(mixed_heads.reshape(tokens, d_model), w_attn.reshape(d_model, d_model), preferred_element_type=jnp.float32)
    residual = (flat_rows.astype(jnp.float32) + attn_out + vec_d[2].astype(jnp.float32)).astype(jnp.bfloat16)
    normed_two = layer_norm(residual, vec_d[3], vec_d[4])
    hidden = jnp.dot(normed_two, w_fc, preferred_element_type=jnp.float32) + b_fc.astype(jnp.float32)
    hidden = jax.nn.gelu(hidden, approximate=True).astype(jnp.bfloat16)
    mlp_out = jnp.dot(hidden, w_proj, preferred_element_type=jnp.float32) + vec_d[5].astype(jnp.float32)
    return (residual.astype(jnp.float32) + mlp_out).astype(jnp.bfloat16).reshape(n_batch, seq_len, d_model)


def stack_forward(hidden_in, layer_ws):
    def scan_body(carry, layer_w):
        return gpt_layer(carry, layer_w), None
    out_h, _ = lax.scan(scan_body, hidden_in, layer_ws)
    return out_h


def copy_pass(x_part, dy_part, layer_ws):
    grad_zero = tuple(jnp.zeros(t.shape, jnp.float32) for t in layer_ws)
    def scan_body(grad_acc, mb_pair):
        x_mb, dy_mb = mb_pair
        y_mb, pull_back = jax.vjp(stack_forward, x_mb, layer_ws)
        dx_mb, dw_mb = pull_back(dy_mb)
        grad_acc = tuple(a + g.astype(jnp.float32) for a, g in zip(grad_acc, dw_mb))
        return grad_acc, (y_mb, dx_mb)
    grad_acc, (y_half, dx_half) = lax.scan(scan_body, grad_zero, (x_part, dy_part))
    return y_half, dx_half, grad_acc


def reference(x_in, dy_out, w_qkv, w_attn, w_fc, w_proj, b_qkv, b_fc, vec_d):
    params = (w_qkv, w_attn, w_fc, w_proj, b_qkv, b_fc, vec_d)
    half_micro = MICRO // 2
    down_ws = tuple(t[:, 0].reshape((LAYERS,) + t.shape[3:]) for t in params)
    up_ws = tuple(t[::-1, 1].reshape((LAYERS,) + t.shape[3:]) for t in params)
    y_down, dx_down, g_down = copy_pass(x_in[:half_micro], dy_out[:half_micro], down_ws)
    y_up, dx_up, g_up = copy_pass(x_in[half_micro:], dy_out[half_micro:], up_ws)
    y_out = jnp.concatenate([y_down, y_up], axis=0)
    dx_in = jnp.concatenate([dx_down, dx_up], axis=0)
    grads = []
    for orig, part_down, part_up in zip(params, g_down, g_up):
        total = (part_down + part_up).reshape((STAGES, LPS) + orig.shape[3:])
        grads.append(jnp.stack([total, total[::-1]], axis=1))
    return (y_out, dx_in, grads[0], grads[1], grads[2], grads[3], grads[4], grads[5], grads[6])
```

```python
import functools
import jax
import jax.numpy as jnp
from jax import lax
from jax.experimental import pallas as pl
from jax.experimental.pallas import tpu as pltpu
from jax.sharding import PartitionSpec as P

EPS = 1e-5
D = 128
F32 = jnp.float32
BF16 = jnp.bfloat16
NEG = -1e30
LOG2E = 1.4426950408889634
GK = 0.7978845608028654
GA = 0.044715


def dot(a, b):
    return lax.dot_general(a, b, (((1,), (0,)), ((), ())), preferred_element_type=F32)


def dot_t(a, b):
    return lax.dot_general(a, b, (((1,), (1,)), ((), ())), preferred_element_type=F32)


def lanes(*xs):
    return jnp.concatenate(xs, axis=1)


def rows(*xs):
    return jnp.concatenate(xs, axis=0)


def csum(x):
    return jnp.sum(x, axis=0, keepdims=True)


def norm_stats(x):
    inv = 1.0 / x.shape[0]
    mean = csum(x) * inv
    cent = x - mean
    var = csum(cent * cent) * inv
    return cent * lax.rsqrt(var + EPS), lax.rsqrt(var + EPS)


def block_diag(a, b):
    z = jnp.zeros_like(a)
    return rows(lanes(a, z), lanes(z, b))


def split_even(x):
    even = (lax.broadcasted_iota(jnp.int32, x.shape, 0) // 8) % 2 == 0
    z = jnp.zeros_like(x)
    return jnp.where(even, x, z), jnp.where(even, z, x)


def widen(e, o, r0, T):
    parts = []
    if r0:
        parts.append(jnp.zeros((r0, 2 * T), BF16))
    parts.append(lanes(e[r0:r0 + 16], o[r0:r0 + 16]))
    if 112 - r0:
        parts.append(jnp.zeros((112 - r0, 2 * T), BF16))
    return rows(*parts)


def row_sum(x):
    return csum(jnp.transpose(x.astype(F32)))


def rnd(x):
    return x.astype(BF16).astype(F32)


def fwd_pair(l, j, T, H, scale, refs):
    (hbuf, qkvbuf, obuf, h1buf, lsebuf, wqkv, wot, w1t, w2t, bias, ubuf) = refs
    m0 = 2 * j
    n1 = []
    for s in range(2):
        x = hbuf[l, m0 + s].astype(F32)
        xh, _ = norm_stats(x)
        n1.append((xh * bias[0:D] + bias[D:256]).astype(BF16))
    n1p = lanes(*n1)
    for c in range(3):
        r = dot(wqkv[c * D:(c + 1) * D], n1p)
        bb = bias[768 + c * D:768 + (c + 1) * D]
        for s in range(2):
            qkvbuf[l, m0 + s, c * D:(c + 1) * D] = (r[:, s * T:(s + 1) * T] + bb).astype(BF16)
    kq = lax.broadcasted_iota(jnp.int32, (T, T), 0) <= lax.broadcasted_iota(jnp.int32, (T, T), 1)
    cs = scale * LOG2E
    ops = []
    for s in range(2):
        qt = qkvbuf[l, m0 + s, 0:D]
        kt = qkvbuf[l, m0 + s, D:256]
        vt = qkvbuf[l, m0 + s, 256:384]
        ops.append((jnp.transpose(kt), split_even(qt), split_even(vt)))
    units = [(s, g4) for g4 in range(H // 4) for s in range(2)]

    def scores(u):
        s, g4 = u
        k_nat, (q_e, q_o), _ = ops[s]
        return [dot(k_nat, widen(q_e, q_o, 16 * g, T)) for g in (2 * g4, 2 * g4 + 1)]

    def probs(u, sg):
        s, g4 = u
        ps = []
        for a in range(2):
            for i in range(2):
                sc = jnp.where(kq, sg[a][:, i * T:(i + 1) * T], NEG)
                m = jnp.max(sc, axis=0, keepdims=True)
                e = jnp.exp2((sc - m) * cs)
                den = csum(e)
                lsebuf[l, m0 + s, pl.ds(4 * g4 + 2 * a + i, 1), :] = m * cs + jnp.log2(den)
                ps.append((e * (1.0 / den)).astype(BF16))
        return ps

    def mix(u, ps):
        s, g4 = u
        v_e, v_o = ops[s][2]
        rhs = rows(lanes(ps[0], ps[2]), lanes(ps[1], ps[3]))
        r0 = 32 * g4
        o4 = dot(lanes(v_e[r0:r0 + 32], v_o[r0:r0 + 32]), rhs)
        obuf[l, m0 + s, r0:r0 + 16] = o4[0:16, 0:T].astype(BF16)
        obuf[l, m0 + s, r0 + 16:r0 + 32] = o4[16:32, T:].astype(BF16)

    AHEAD = 2
    q = {}
    for i in range(AHEAD):
        q[i] = scores(units[i])
    for i, u in enumerate(units):
        ps = probs(u, q.pop(i))
        if i + AHEAD < len(units):
            q[i + AHEAD] = scores(units[i + AHEAD])
        mix(u, ps)
    op = lanes(obuf[l, m0], obuf[l, m0 + 1])
    ao = dot(wot[...], op)
    n2 = []
    for s in range(2):
        h1 = (hbuf[l, m0 + s].astype(F32) + ao[:, s * T:(s + 1) * T] + bias[256:384]).astype(BF16)
        h1buf[l, m0 + s] = h1
        xh, _ = norm_stats(h1.astype(F32))
        n2.append((xh * bias[384:512] + bias[512:640]).astype(BF16))
    n2p = lanes(*n2)
    nf = w1t.shape[0] // D
    for c in range(nf):
        r = dot(w1t[c * D:(c + 1) * D], n2p)
        bb = bias[1152 + c * D:1152 + (c + 1) * D]
        for s in range(2):
            z = r[:, s * T:(s + 1) * T] + bb
            t = jnp.tanh(GK * (z + GA * (z * z * z)))
            ubuf[c * D:(c + 1) * D, s * T:(s + 1) * T] = (0.5 * z * (1.0 + t)).astype(BF16)
    y = dot(w2t[...], ubuf[...])
    for s in range(2):
        hbuf[l + 1, m0 + s] = (h1buf[l, m0 + s].astype(F32) + y[:, s * T:(s + 1) * T] + bias[640:768]).astype(BF16)


def acc_pair(acc, r, T):
    acc[...] = acc[...] + rnd(r[:, :T]) + rnd(r[:, T:])


def acc_row(acc, i, w, row):
    acc[i:i + 1, 0:w] = acc[i:i + 1, 0:w] + rnd(row)


def bwd_pair(l, j, T, H, scale, refs):
    (hbuf, qkvbuf, obuf, h1buf, lsebuf, dbuf, wqkvn, wo, w1t, w1, w2, bias, ubuf, dhbuf, gqkv, gwo, gw1t, gw2, gvec, dqkvb) = refs
    m0 = 2 * j
    nf = w1t.shape[0] // D
    n2, xh2, r2 = [], [], []
    for s in range(2):
        xh, r = norm_stats(h1buf[l, m0 + s].astype(F32))
        n2.append((xh * bias[384:512] + bias[512:640]).astype(BF16))
    n2p = lanes(*n2)
    dyp = lanes(dbuf[m0], dbuf[m0 + 1])
    for c in range(nf):
        r = dot(w1t[c * D:(c + 1) * D], n2p)
        du = dot(w2[c * D:(c + 1) * D], dyp)
        bb = bias[1152 + c * D:1152 + (c + 1) * D]
        for s in range(2):
            z = r[:, s * T:(s + 1) * T] + bb
            z2 = z * z
            t = jnp.tanh(z * (GK + (GK * GA) * z2))
            ht = 0.5 * t + 0.5
            ubuf[c * D:(c + 1) * D, s * T:(s + 1) * T] = (z * ht).astype(BF16)
            gp = ht + (z * (0.5 - 0.5 * (t * t))) * (GK + (3 * GK * GA) * z2)
            dz = rnd(du[:, s * T:(s + 1) * T]) * gp
            dhbuf[c * D:(c + 1) * D, s * T:(s + 1) * T] = dz.astype(BF16)
            acc_row(gvec, 16 + c, D, row_sum(dz))
    one_row = jnp.concatenate([jnp.ones((16, 2 * T), BF16)], axis=0)
    acc_pair(gw2, dot_t(ubuf[...], block_diag(dbuf[m0], dbuf[m0 + 1])), T)
    for s in range(2):
        acc_row(gvec, 5, D, row_sum(dbuf[m0 + s]))
    acc_pair(gw1t, dot_t(dhbuf[...], block_diag(n2[0], n2[1])), T)
    dn2 = dot(w1[...], dhbuf[...])
    dres = []
    for s in range(2):
        xh, r = norm_stats(h1buf[l, m0 + s].astype(F32))
        d = rnd(dn2[:, s * T:(s + 1) * T])
        acc_row(gvec, 3, D, row_sum(d * xh))
        acc_row(gvec, 4, D, row_sum(d))
        dx = d * bias[384:512]
        a = csum(dx) * (1.0 / D)
        b = csum(dx * xh) * (1.0 / D)
        dres.append((dbuf[m0 + s].astype(F32) + r * (dx - a - xh * b)).astype(BF16))
        acc_row(gvec, 2, D, row_sum(dres[s]))
    drp = lanes(*dres)
    acc_pair(gwo, dot_t(lanes(obuf[l, m0], obuf[l, m0 + 1]), block_diag(*dres)), T)
    dop = dot(wo[...], drp).astype(BF16)
    kq = lax.broadcasted_iota(jnp.int32, (T, T), 0) <= lax.broadcasted_iota(jnp.int32, (T, T), 1)
    cs = scale * LOG2E
    ops = []
    z16 = jnp.zeros((16, T), BF16)
    for s in range(2):
        qt = qkvbuf[l, m0 + s, 0:D]
        kt = qkvbuf[l, m0 + s, D:256]
        vt = qkvbuf[l, m0 + s, 256:384]
        do = dop[:, s * T:(s + 1) * T]
        prod = do.astype(F32) * obuf[l, m0 + s].astype(F32)
        ops.append((qt, do, prod, jnp.transpose(kt), jnp.transpose(vt), split_even(qt), split_even(do), split_even(kt)))
    units = [(s, g4) for g4 in range(H // 4) for s in range(2)]

    def scores(u):
        s, g4 = u
        _, _, _, k_nat, v_nat, (q_e, q_o), (d_e, d_o), _ = ops[s]
        return [(dot(k_nat, widen(q_e, q_o, 16 * g, T)), dot(v_nat, widen(d_e, d_o, 16 * g, T))) for g in (2 * g4, 2 * g4 + 1)]

    def probs(u, sg):
        s, g4 = u
        prod = ops[s][2]
        ps, dss = [], []
        for a in range(2):
            for i in range(2):
                h = 4 * g4 + 2 * a + i
                lse = lsebuf[l, m0 + s, pl.ds(h, 1), :]
                p = jnp.exp2(jnp.where(kq, sg[a][0][:, i * T:(i + 1) * T] * cs - lse, NEG))
                dd = csum(prod[8 * h:8 * h + 8])
                ps.append(p.astype(BF16))
                dss.append((p * (sg[a][1][:, i * T:(i + 1) * T] - dd)).astype(BF16))
        return ps, dss

    def mix(u, pd):
        s, g4 = u
        ps, dss = pd
        qt, do = ops[s][0], ops[s][1]
        k_e, k_o = ops[s][7]
        r0 = 32 * g4
        tp = rows(lanes(ps[0], ps[2]), lanes(ps[1], ps[3]))
        tds = rows(lanes(dss[0], dss[2]), lanes(dss[1], dss[3]))

        def half(x):
            return rows(lanes(x[r0:r0 + 16], z16), lanes(z16, x[r0 + 16:r0 + 32]))
        rv = dot_t(half(do), tp)
        rk = dot_t(half(qt), tds)
        rq = dot(lanes(k_e[r0:r0 + 32], k_o[r0:r0 + 32]), tds)
        dvt = rows(rv[0:8, :T], rv[8:16, T:], rv[16:24, :T], rv[24:32, T:])
        dkt = rows(rk[0:8, :T], rk[8:16, T:], rk[16:24, :T], rk[24:32, T:]) * scale
        dqt = rows(rq[0:16, :T], rq[16:32, T:]) * scale
        dqkvb[r0:r0 + 32, s * T:(s + 1) * T] = dqt.astype(BF16)
        dqkvb[D + r0:D + r0 + 32, s * T:(s + 1) * T] = dkt.astype(BF16)
        dqkvb[256 + r0:256 + r0 + 32, s * T:(s + 1) * T] = dvt.astype(BF16)

    AHEAD = 2
    q = {}
    for i in range(AHEAD):
        q[i] = scores(units[i])
    for i, u in enumerate(units):
        ps = probs(u, q.pop(i))
        if i + AHEAD < len(units):
            q[i + AHEAD] = scores(units[i + AHEAD])
        mix(u, ps)
    for s in range(2):
        for c in range(3):
            acc_row(gvec, 8 + c, D, row_sum(dqkvb[c * D:(c + 1) * D, s * T:(s + 1) * T]))
    dn1 = dot(wqkvn[...], dqkvb[...])
    n1 = []
    for s in range(2):
        xh, r = norm_stats(hbuf[l, m0 + s].astype(F32))
        n1.append((xh * bias[0:D] + bias[D:256]).astype(BF16))
        d = rnd(dn1[:, s * T:(s + 1) * T])
        acc_row(gvec, 0, D, row_sum(d * xh))
        acc_row(gvec, 1, D, row_sum(d))
        dx = d * bias[0:D]
        a = csum(dx) * (1.0 / D)
        b = csum(dx * xh) * (1.0 / D)
        dbuf[m0 + s] = (dres[s].astype(F32) + r * (dx - a - xh * b)).astype(BF16)
    acc_pair(gqkv, dot_t(dqkvb[...], block_diag(n1[0], n1[1])), T)


GROWS = 1560
MESH = pl.DeviceIdType.MESH


def flip(i, bit):
    return i + bit - 2 * bit * ((i // bit) % 2)


def fold(i, n):
    return jnp.where(2 * i < n, i, n - 1 - i)


def role_of(me, l, n):
    a, b = fold(me, n), fold(l, n)
    return (a + b) % 2 + 2 * ((a // 2 + b // 2) % 2)


def kernel(n, x_ref, dy_ref, wq_in, wa_in, wf_in, wp_in, ws_in, y_ref, dx_ref, oq, oa, of, op, ov,
           hbuf, qkvbuf, obuf, h1buf, lsebuf, dbuf, wot, w1t, w2t, w1c, wqkvn, bias, ubuf, dhbuf, dqkvb, gw1t,
           wq, wa, wf, wp, ws, gsum, r1, r2, r3,
           loc_sem, wsend, wrecv, s1, s2, s3, q1, q2, q3):
    me = lax.axis_index('pp')
    mate, side, far = flip(me, 1), flip(me, 2), n - 1 - me
    L = n
    n_mb = x_ref.shape[0]
    T = x_ref.shape[-2]
    H = 16
    scale = 8 ** -0.5
    nf = w1t.shape[0] // D
    ins = (wq_in, wa_in, wf_in, wp_in, ws_in)
    alls = (wq, wa, wf, wp, ws)
    lo, hi = fold(me, n), n - 1 - fold(me, n)

    def copy_no(l):
        return jnp.where(l == me, 0, 1)

    def own_copy(c, l, k):
        return pltpu.make_async_copy(ins[k].at[c], alls[k].at[l], loc_sem.at[c, k])

    def send_own(l, dest, slot, k):
        return pltpu.make_async_remote_copy(ins[k].at[copy_no(l)], alls[k].at[l], wsend.at[slot, k], wrecv.at[l, k],
                                            device_id={'pp': dest}, device_id_type=MESH)

    def relay(l, slot, k):
        return pltpu.make_async_remote_copy(alls[k].at[l], alls[k].at[l], wsend.at[slot, k], wrecv.at[l, k],
                                            device_id={'pp': mate}, device_id_type=MESH)

    arrays = range(len(ins))
    for k in arrays:
        own_copy(0, me, k).start()
        own_copy(1, far, k).start()
    bar = pltpu.get_barrier_semaphore()
    for peer in (mate, side, far):
        pl.semaphore_signal(bar, inc=1, device_id={'pp': peer}, device_id_type=MESH)
    pl.semaphore_wait(bar, 3)
    for k in arrays:
        send_own(lo, mate, 0, k).start()

    @pl.when(lo != 1)
    def _():
        for k in arrays:
            send_own(lo, side, 2, k).start()
        for k in arrays:
            send_own(hi, side, 3, k).start()
    for k in arrays:
        send_own(hi, mate, 1, k).start()

    def load_x(m, _):
        hbuf[0, m] = jnp.transpose(x_ref[m].astype(F32)).astype(BF16)
        dbuf[m] = jnp.transpose(dy_ref[m].astype(F32)).astype(BF16)
        return 0
    lax.fori_loop(0, n_mb, load_x, 0)
    for k in arrays:
        own_copy(0, me, k).wait()
        own_copy(1, far, k).wait()

    side_lo, side_hi = fold(side, n), n - 1 - fold(side, n)

    def arrive(l):
        @pl.when((l == side_lo) | (l == side_hi))
        def _():
            for k in arrays:
                relay(l, 4, k).wait_recv()

            @pl.when(l == side_lo)
            def _():
                for k in arrays:
                    relay(l, 4, k).start()

            @pl.when(l == side_hi)
            def _():
                for k in arrays:
                    relay(l, 5, k).start()

        @pl.when((l != lo) & (l != hi) & (l != side_lo) & (l != side_hi))
        def _():
            for k in arrays:
                relay(l, 4, k).wait_recv()

    def set_bias(l):
        for i in range(13):
            row = ws[l, pl.ds(i, 1), :].astype(F32)
            bias[i * D:(i + 1) * D] = jnp.transpose(jnp.broadcast_to(row, (D, D)))

    half = n_mb // 4

    def fwd_layer(l, _):
        arrive(l)

        @pl.when((l == 0) & (lo == 1))
        def _():
            for k in arrays:
                send_own(lo, side, 2, k).start()
            for k in arrays:
                send_own(hi, side, 3, k).start()
        set_bias(l)
        wot[...] = jnp.transpose(wa[l])
        for c in range(nf):
            w1t[c * D:(c + 1) * D] = jnp.transpose(wf[l, :, c * D:(c + 1) * D])
            w2t[:, c * D:(c + 1) * D] = jnp.transpose(wp[l, c * D:(c + 1) * D])

        def body(j, _):
            fwd_pair(l, j, T, H, scale, (hbuf, qkvbuf, obuf, h1buf, lsebuf, wq.at[l], wot, w1t, w2t, bias, ubuf))
            return 0
        lax.fori_loop(0, n_mb // 2, body, 0)
        return 0
    lax.fori_loop(0, L, fwd_layer, 0)

    def put_y(m, _):
        y_ref[m] = jnp.transpose(hbuf[L, m].astype(F32)).astype(BF16)
        return 0
    lax.fori_loop(0, n_mb, put_y, 0)

    def slot_of(l):
        return jnp.where(2 * l < n, 0, 1)

    def hop1(l, role):
        k = role // 2 * 2 + slot_of(l)
        return pltpu.make_async_remote_copy(gsum.at[l], r1.at[k], s1.at[k], q1.at[k], device_id={'pp': mate}, device_id_type=MESH)

    def hop2(l):
        k = slot_of(l)
        return pltpu.make_async_remote_copy(gsum.at[l], r2.at[k], s2.at[k], q2.at[k], device_id={'pp': side}, device_id_type=MESH)

    def hop3(l):
        k = slot_of(l)
        return pltpu.make_async_remote_copy(gsum.at[l], r3.at[k], s3.at[k], q3.at[k], device_id={'pp': far}, device_id_type=MESH)

    def add_rows(l, buf, k):
        def step(i, _):
            at = pl.ds(pl.multiple_of(i * (GROWS // 5), 8), GROWS // 5)
            gsum[l, at] = gsum[l, at] + buf[k, at]
            return 0
        lax.fori_loop(0, 5, step, 0)

    def first(l):
        role = role_of(me, l, n)

        @pl.when(role % 2 == 1)
        def _():
            hop1(l, role).start()

    def second(l):
        role = role_of(me, l, n)

        @pl.when(role % 2 == 0)
        def _():
            hop1(l, role).wait_recv()
            add_rows(l, r1, role // 2 * 2 + slot_of(l))

        @pl.when(role == 2)
        def _():
            hop2(l).start()

    def third(l):
        @pl.when(role_of(me, l, n) == 0)
        def _():
            hop2(l).wait_recv()
            add_rows(l, r2, slot_of(l))
            hop3(l).start()

    def last(l):
        @pl.when(role_of(me, l, n) == 0)
        def _():
            k = slot_of(l)
            c = copy_no(l)
            hop3(l).wait_recv()

            def total(a, size):
                at = pl.ds(a, size)
                return gsum[l, at] + r3[k, at]
            oq[c] = total(0, 384)
            oa[c] = total(384, D)
            for i in range(nf):
                of[c, :, i * D:(i + 1) * D] = total(512 + i * D, D)
            op[c] = total(1024, 512)
            ov[c] = total(1536, 24)

    def bwd_layer(i, _):
        l = L - 1 - i
        set_bias(l)
        for c in range(nf):
            w1t[c * D:(c + 1) * D] = jnp.transpose(wf[l, :, c * D:(c + 1) * D])
        for c in range(3):
            wqkvn[:, c * D:(c + 1) * D] = jnp.transpose(wq[l, c * D:(c + 1) * D])
        gw1t[...] = jnp.zeros_like(gw1t)
        gsum[l] = jnp.zeros((GROWS, D), F32)

        @pl.when(i >= 1)
        def _():
            first(l + 1)

        @pl.when(i >= 3)
        def _():
            third(l + 3)

        def body(j, _):
            g = gsum.at[l]
            bwd_pair(l, j, T, H, scale, (hbuf, qkvbuf, obuf, h1buf, lsebuf, dbuf, wqkvn, wa.at[l], w1t, wf.at[l], wp.at[l], bias, ubuf, dhbuf,
                                         g.at[0:384], g.at[384:512], gw1t, g.at[1024:1536], g.at[1536:1560], dqkvb))
            return 0

        lax.fori_loop(0, half, body, 0)

        @pl.when(i >= 1)
        def _():
            second(l + 1)

        @pl.when(i >= 4)
        def _():
            last(l + 4)
        lax.fori_loop(half, n_mb // 2, body, 0)
        for c in range(nf):
            gsum[l, 512 + c * D:640 + c * D] = jnp.transpose(gw1t[c * D:(c + 1) * D])
        return 0
    lax.fori_loop(0, L, bwd_layer, 0)

    def put_dx(m, _):
        dx_ref[m] = jnp.transpose(dbuf[m].astype(F32)).astype(BF16)
        return 0
    lax.fori_loop(0, n_mb, put_dx, 0)
    first(0)
    third(2)
    last(3)
    second(0)
    third(1)
    last(2)
    third(0)
    last(1)
    last(0)

    for k in arrays:
        send_own(lo, mate, 0, k).wait_send()
        send_own(hi, mate, 1, k).wait_send()
        send_own(lo, side, 2, k).wait_send()
        send_own(hi, side, 3, k).wait_send()
        relay(side_lo, 4, k).wait_send()
        relay(side_hi, 5, k).wait_send()

    def sent(l, _):
        role = role_of(me, l, n)

        @pl.when(role % 2 == 1)
        def _():
            hop1(l, role).wait_send()

        @pl.when(role == 2)
        def _():
            hop2(l).wait_send()

        @pl.when(role == 0)
        def _():
            hop3(l).wait_send()
        return 0
    lax.fori_loop(0, L, sent, 0)


def train_step(n, x, dy, wq, wa, wf, wp, ws):
    n_mb, T, _ = x.shape
    L = n
    V = pltpu.VMEM
    vm = pl.BlockSpec(memory_space=pltpu.VMEM)
    hbm = pl.BlockSpec(memory_space=pl.ANY)
    DMA = pltpu.SemaphoreType.DMA
    big = (GROWS, D)
    return pl.pallas_call(
        functools.partial(kernel, n),
        out_shape=(jax.ShapeDtypeStruct(x.shape, BF16), jax.ShapeDtypeStruct(x.shape, BF16)) + tuple(
            jax.ShapeDtypeStruct(t.shape, F32) for t in (wq, wa, wf, wp)) + (jax.ShapeDtypeStruct((2, 24, D), F32),),
        in_specs=[vm] * 2 + [hbm] * 5,
        out_specs=(vm,) * 7,
        scratch_shapes=[
            V((L + 1, n_mb, D, T), BF16), V((L, n_mb, 384, T), BF16), V((L, n_mb, D, T), BF16), V((L, n_mb, D, T), BF16),
            V((L, n_mb, 16, T), F32), V((n_mb, D, T), BF16),
            V((D, D), BF16), V((512, D), BF16), V((D, 512), BF16), V((8, D), BF16), V((D, 384), BF16),
            V((13 * D, D), F32), V((512, 2 * T), BF16), V((512, 2 * T), BF16), V((384, 2 * T), BF16),
            V((512, D), F32),
            V((L,) + wq.shape[1:], BF16), V((L,) + wa.shape[1:], BF16), V((L,) + wf.shape[1:], BF16), V((L,) + wp.shape[1:], BF16), V((L,) + ws.shape[1:], BF16),
            V((L,) + big, F32), V((4,) + big, F32), V((2,) + big, F32), V((2,) + big, F32),
            DMA((2, 5)), DMA((6, 5)), DMA((L, 5)), DMA((4,)), DMA((2,)), DMA((2,)), DMA((4,)), DMA((2,)), DMA((2,))],
        compiler_params=pltpu.CompilerParams(vmem_limit_bytes=62 * 1024 * 1024, collective_id=0, has_side_effects=True),
        name="train_step",
    )(x, dy, wq, wa, wf, wp, ws)


def solution(mesh):
    n = mesh.shape['pp']
    data_spec = P(('dp', 'pp'))
    weight_spec = P('pp')

    def per_device(x_loc, dy_loc, w_qkv, w_attn, w_fc, w_proj, b_qkv, b_fc, vec_d):
        wq = w_qkv.transpose(0, 1, 2, 4, 5, 6, 3).reshape(2, 384, D)
        ws = jnp.concatenate([vec_d.reshape(2, 6, D), b_qkv.reshape(2, 3, D), b_fc.reshape(2, 4, D), jnp.zeros((2, 3, D), BF16)], axis=1)
        y, dx, gq, ga, gf, gp, gv = train_step(n, x_loc[:, 0], dy_loc[:, 0], wq, w_attn.reshape(2, D, D), w_fc.reshape(2, D, 512), w_proj.reshape(2, 512, D), ws)
        gq = gq.reshape(1, 2, 1, 3, 16, 8, D).transpose(0, 1, 2, 6, 3, 4, 5)
        return (y[:, None], dx[:, None], gq, ga.reshape(w_attn.shape), gf.reshape(w_fc.shape), gp.reshape(w_proj.shape),
                gv[:, 8:11].reshape(b_qkv.shape), gv[:, 16:20].reshape(b_fc.shape), gv[:, 0:6].reshape(vec_d.shape))

    return jax.shard_map(per_device, mesh=mesh, in_specs=(data_spec, data_spec) + (weight_spec,) * 7, out_specs=(data_spec,) * 9, check_vma=False)
```
